32 devices in a mesh: rp: 2 (over x), pb: 16 (over z, y, core).
Axes of the slice: x: 2, y: 2, z: 4, core: 2. Of those that a mesh axis runs over, the one named last changes fastest.
Arguments:
- wannier_g: bfloat16 [2, 1024, 32, 1152], P(None, 'rp', 'pb'), may hold values from -0.19921875 to 0.19921875
- rp_coords: int32 [3, 1024], replicated, may hold values from -8 to 8
- q_coords: int32 [3, 64], P(None, ('rp', 'pb')), may hold values from 0 to 15
- k_index: int32 [1], replicated, may hold values from 0 to 7
- k_vectors: bfloat16 [8, 2, 32, 32], replicated, may hold values from -0.75 to 0.75
- kq_vectors: bfloat16 [64, 2, 32, 32], P(('rp', 'pb')), may hold values from -0.75 to 0.75
- modes: bfloat16 [64, 2, 36, 36], P(('rp', 'pb')), may hold values from -0.75 to 0.75
Outputs:
- rotated: float32 [64, 2, 32, 1152], P(('rp', 'pb'))
The draws below stay inside these ranges and needn't reach their ends.
All inputs are finite; a program needn't handle non-finite values.
Results may differ from the reference program's by a relative error of at most 0.0054.
Values may be sent and summed in bfloat16 or wider, within the bound.
A program may use at most 64 MiB of HBM per device.

```python
import math
import jax
import jax.numpy as jnp
from jax import lax

NB = 32
NM = 36
NR = 1024
NK = 16
KB = 8
Q_DEV = 2
Q = 64
N_RP = 2
N_PB = 16


def with_ends(entries, stream_key, least, largest):
    longest = entries.shape.index(max(entries.shape))
    spots = []
    for shift in (0, 1):
        where = [jax.random.randint(jax.random.fold_in(stream_key, axis), (), 0, length) for axis, length in enumerate(entries.shape)]
        where[longest] = (where[longest] + shift) % entries.shape[longest]
        spots.append(tuple(where))
    return entries.at[spots[0]].set(least).at[spots[1]].set(largest)


def levels(own_key, dims, cuts, low, largest):
    def one(axis_at, parts):
        heights = jax.random.uniform(jax.random.fold_in(jax.random.fold_in(own_key, 6), axis_at), (parts,), jnp.float32, low / len(cuts), largest / len(cuts))
        return jnp.repeat(jnp.exp(heights), dims[axis_at] // parts).reshape((-1,) + (1,) * (len(dims) - axis_at - 1))

    factor_of = one(*cuts[0])
    for cut in cuts[1:]:
        factor_of = factor_of * one(*cut)
    return factor_of


def centred(key, extent, width, most, split=(), dtype=jnp.bfloat16):
    values = width * jax.random.normal(key, extent, jnp.float32)
    if split:
        values = values * levels(key, extent, split, -0.22, 0.18)
    return jnp.clip(values, -most, most).astype(dtype)


def setup_inputs(seed: int = 0) -> dict:
    streams_of = jax.random.split(jax.random.key(seed), 8)
    return {
        "wannier_g": centred(streams_of[0], (2, NR, NB, NB * NM), 0.03, 0.19921875, ((1, 2), (2, 16))),
        "rp_coords": with_ends(jax.random.randint(streams_of[1], (3, NR), -8, 9), jax.random.fold_in(streams_of[1], 1), -8, 8).astype(jnp.int32),
        "q_coords": with_ends(jax.random.randint(streams_of[2], (3, Q), 0, NK), jax.random.fold_in(streams_of[2], 1), 0, NK - 1).astype(jnp.int32),
        "k_index": jax.random.randint(streams_of[3], (1,), 0, KB).astype(jnp.int32),
        "k_vectors": centred(streams_of[4], (KB, 2, NB, NB), (2 * NB) ** -0.5, 0.75),
        "kq_vectors": centred(streams_of[5], (Q, 2, NB, NB), (2 * NB) ** -0.5, 0.75, ((0, 32),)),
        "modes": centred(streams_of[6], (Q, 2, NM, NM), (2 * NM) ** -0.5, 0.75, ((0, 32),)),
    }


def phases(q_rows, r_coords):
    turns = jnp.mod(jnp.sum(q_rows[:, :, None] * r_coords[:, None, :], axis=0), NK)
    angle = turns.astype(jnp.float32) * (2.0 * math.pi / NK)
    cosine = jnp.cos(angle).astype(jnp.bfloat16)
    sine = jnp.sin(angle).astype(jnp.bfloat16)
    return jnp.concatenate([cosine, -sine], axis=1), jnp.concatenate([sine, cosine], axis=1)


def rotate(fourier, mode_vecs, unit, kq_vecs):
    count = fourier.shape[0]
    field = fourier.reshape(count, 2, NB, NB, NM).astype(jnp.float32)
    e_real, e_imag = mode_vecs[:, 0], mode_vecs[:, 1]
    e_block = jnp.stack([jnp.stack([e_real, e_imag], 2), jnp.stack([-e_imag, e_real], 2)], 1).astype(jnp.float32)
    by_mode = jnp.einsum("qcmnv,qcvdu->qdmnu", field, e_block).astype(jnp.bfloat16)
    u_real, u_imag = unit[0], unit[1]
    u_block = jnp.stack([jnp.stack([u_real, u_imag], 1), jnp.stack([-u_imag, u_real], 1)], 0).astype(jnp.float32)
    by_band = jnp.einsum("qcmnu,cndj->qdmju", by_mode.astype(jnp.float32), u_block).astype(jnp.bfloat16)
    v_real, v_imag = kq_vecs[:, 0], kq_vecs[:, 1]
    v_block = jnp.stack([jnp.stack([v_real, -v_imag], 2), jnp.stack([v_imag, v_real], 2)], 1).astype(jnp.float32)
    result = jnp.einsum("qcmju,qcmdi->qdiju", by_band.astype(jnp.float32), v_block)
    return result.reshape(count, 2, NB, NB * NM)


def reference(wannier_g, rp_coords, q_coords, k_index, k_vectors, kq_vectors, modes):
    blocks = N_RP * N_PB
    right = wannier_g.reshape(2 * NR, NB * NB * NM)
    unit = lax.dynamic_index_in_dim(k_vectors, k_index[0], 0, keepdims=False)
    q_blocks = q_coords.reshape(3, blocks, Q_DEV).transpose(1, 0, 2)
    mode_blocks = modes.reshape(blocks, Q_DEV, 2, NM, NM)
    kq_blocks = kq_vectors.reshape(blocks, Q_DEV, 2, NB, NB)

    def one_block(items):
        q_rows, mode_vecs, kq_vecs = items
        left_real, left_imag = phases(q_rows, rp_coords)
        f_real = jnp.dot(left_real, right, preferred_element_type=jnp.float32).astype(jnp.bfloat16)
        f_imag = jnp.dot(left_imag, right, preferred_element_type=jnp.float32).astype(jnp.bfloat16)
        fourier = jnp.stack([f_real, f_imag], 1)
        return rotate(fourier, mode_vecs, unit, kq_vecs)

    result = lax.map(one_block, (q_blocks, mode_blocks, kq_blocks))
    return result.reshape(Q, 2, NB, NB * NM)
```

```python
import functools

import jax
import jax.numpy as jnp
import numpy as np
from jax import lax
from jax.experimental import pallas as pl
from jax.experimental.pallas import tpu as pltpu
from jax.sharding import PartitionSpec as P

NK = 16
LANES = 128
MESH = pl.DeviceIdType.MESH
F32 = jnp.float32
BF16 = jnp.bfloat16
ROUND = 1.5 * 2.0**23 * NK
ODD = np.linalg.solve(
    np.array([[h, h**3, h**5, h**7] for h in (1.0, 2.0, 3.0, 4.0)]),
    np.sin(np.pi * np.arange(1, 5) / 8.0),
)


def dot(a, b, dims=((1,), (0,))):
    return lax.dot_general(a, b, (dims, ((), ())), preferred_element_type=F32)


def iota(shape, axis):
    return lax.broadcasted_iota(jnp.int32, shape, axis)


def picks(rows, cols, hit):
    return jnp.where(hit(iota((rows, cols), 0), iota((rows, cols), 1)), 1.0, 0.0).astype(BF16)


def wave(t):
    h = NK // 4 - jnp.abs(t - ((t + ROUND) - ROUND))
    s = h * h
    return h * (ODD[0] + s * (ODD[1] + s * (ODD[2] + s * ODD[3])))


def wrapped(a, b, size):
    c = a + b
    return jnp.where(c >= size, c - size, c)


def cuts(tiles):
    if tiles < 8:
        return [tiles]
    rest = tiles - 2
    return [1] + [rest // 3 + (k == 1) * (rest % 3) for k in range(3)] + [1]


def kernel(
    cfg, g_hbm, rp_hbm, q_hbm, k_hbm, kv_hbm, v_hbm, e_hbm, o_ref,
    g_buf, q_ref, k_ref, rp_ref, kv_ref, v_ref, e_ref, qrow, q_all, xsend, xrecv, own_f, red, recv,
    w_buf, rmat, v_left,
    g_sem, in_sem, qs_sem, qr_sem, xs_sem, xr_sem, s_sem, r_sem,
):
    n_rp, n_pb, qd, local, M, cols, bands, nu, RB, KL, paired = cfg
    n = n_rp * n_pb
    ip, ib = lax.axis_index("rp"), lax.axis_index("pb")
    me = ip * n_pb + ib
    depth = local * M
    tiles = cols // LANES
    nh = n_pb // 2
    rows = nh * RB
    near0 = (ib // nh) * nh
    far0 = nh - near0
    starts = (far0, near0)

    def group(g, act):
        def one(k, c):
            act(wrapped(ib - near0, k, nh) + starts[g])
            return c

        lax.fori_loop(g, nh, one, 0)

    def to_all(act):
        for dp in range(1, n_rp):
            for g in range(2):
                p = wrapped(ip, dp, n_rp)
                if g == 1:
                    act(p, ib)
                group(g, lambda b, p=p: act(p, b))
        for g in range(2):
            group(g, lambda b: act(ip, b))

    barrier = pltpu.get_barrier_semaphore()
    to_all(
        lambda p, b: pl.semaphore_signal(barrier, inc=1, device_id=(p, b), device_id_type=MESH)
    )

    inputs = [
        pltpu.make_async_copy(a, b, in_sem.at[k])
        for k, (a, b) in enumerate(
            (
                (q_hbm, q_ref), (k_hbm, k_ref), (rp_hbm, rp_ref), (kv_hbm, kv_ref),
                (v_hbm, v_ref), (e_hbm, e_ref),
            )
        )
    ]
    for c in inputs:
        c.start()
    flat = g_hbm.reshape(2 * depth, cols) if paired else g_hbm
    for t in range(tiles):
        src = flat.at[:, pl.ds(LANES * t, LANES)]
        pltpu.make_async_copy(src, g_buf.at[t], g_sem).start()

    inputs[0].wait()
    lane = iota((1, LANES), 1)
    row = jnp.zeros((1, LANES), jnp.int32)
    for d in range(3):
        for j in range(qd):
            row = jnp.where(lane // M == d * qd + j, q_ref[j, d], row)
    qrow[...] = (row & (NK - 1)).astype(F32)
    q_all[me] = qrow[...]

    pl.semaphore_wait(barrier, n - 1)

    def q_copy(p, b, kind):
        return pltpu.make_async_remote_copy(
            src_ref=qrow, dst_ref=q_all.at[me], send_sem=qs_sem,
            recv_sem=qr_sem.at[kind], device_id=(p, b), device_id_type=MESH,
        )

    for dp in range(1, n_rp):
        p = wrapped(ip, dp, n_rp)
        group(0, lambda b, p=p: q_copy(p, b, 0).start())
    group(0, lambda b: q_copy(ip, b, 1).start())
    for dp in range(1, n_rp):
        p = wrapped(ip, dp, n_rp)
        q_copy(p, ib, 1).start()
        group(1, lambda b, p=p: q_copy(p, b, 1).start())
    group(1, lambda b: q_copy(ip, b, 1).start())
    partner = (wrapped(ip, 1 % n_rp, n_rp), ib)

    def q_waits(count, kind):
        part = q_all.at[pl.ds(0, count)]
        return pltpu.make_async_remote_copy(
            src_ref=part, dst_ref=part, send_sem=qs_sem, recv_sem=qr_sem.at[kind],
            device_id=partner, device_id_type=MESH,
        )

    for c in inputs[1:]:
        c.wait()

    own = rp_ref[:, pl.ds(pl.multiple_of(ip * local, LANES), local)] & (NK - 1)
    spread = picks(local, depth, lambda a, b: a == b // M)
    own = dot(own.astype(F32).astype(BF16), spread)
    at = iota((KL, depth), 0)
    same = at % M == iota((KL, depth), 1) % M
    which = at // (qd * M)
    big = jnp.zeros((KL, depth), F32)
    for d in range(3):
        big = jnp.where(which == d, own[d : d + 1, :], big)
    big = jnp.where(same, big, 0.0)
    first = 3 * qd * M
    part = (at - first) // M
    for c in range(2):
        turn = (0.0, 3.0 * NK / 4) if c == 0 else (NK / 4, 0.0)
        turn = jnp.where(same, jnp.where(part == 0, turn[0], turn[1]), NK / 4)
        turn = jnp.where(at < first + 2 * M, turn, 0.0)
        rmat[:, c * depth : (c + 1) * depth] = jnp.where(at < first, big, turn).astype(BF16)

    slot = iota((RB, LANES), 0)
    at = iota((RB, LANES), 1)
    takes = (at < first) & ((at // M) % qd == slot // (2 * M)) & (at % M == slot % M)
    const = jnp.where((slot < qd * 2 * M) & (at - first == slot % (2 * M)), 1.0, 0.0)

    half = n_pb * RB
    slot = iota((bands, half), 1) % RB
    m_of = (iota((bands, half), 1) // RB) * M + slot % M
    pick_m = jnp.where(iota((bands, half), 0) == m_of, 1.0, 0.0).astype(BF16)
    real_in = (slot // M) % 2 == 0
    for q in range(qd):
        a_r, a_i = [dot(v_ref[q, c], pick_m, ((0,), (0,))) for c in range(2)]
        mine = slot // (2 * M) == q
        top = jnp.where(mine, jnp.where(real_in, a_r, a_i), 0.0)
        low = jnp.where(mine, jnp.where(real_in, -a_i, a_r), 0.0)
        v_left[4 * bands * q : 4 * bands * (q + 1), :] = jnp.concatenate(
            [top, low, -low, top], 0
        ).astype(BF16)

    unit = kv_ref[k_ref[0, 0]]
    of_band_t = picks(bands, cols, lambda b, a: (a >= nu * b) & (a < nu * b + nu))
    of_mode_t = picks(nu, cols, lambda b, a: (a - b + nu * bands) % nu == 0)
    u_right = [dot(unit[c], of_band_t).astype(BF16) for c in range(2)]
    e_right = [[dot(e_ref[q, :, c, :], of_mode_t).astype(BF16) for c in range(2)] for q in range(qd)]

    def combine(t):
        first = t * LANES
        of_band = picks(LANES, bands, lambda a, b: (a + first >= nu * b) & (a + first < nu * b + nu))
        of_mode = picks(LANES, nu, lambda a, b: (a + first - b + nu * bands) % nu == 0)
        ur, ui = [dot(of_band, m) for m in u_right]
        for q in range(qd):
            er, ei = [dot(of_mode, m) for m in e_right[q]]
            w_buf[q, 2 * first : 2 * first + LANES, :] = (ur * er - ui * ei).astype(BF16)
            w_buf[q, 2 * first + LANES : 2 * first + 2 * LANES, :] = (ur * ei + ui * er).astype(BF16)

    todo = list(range(tiles))

    def combine_some(most):
        for _ in range(min(most, len(todo))):
            combine(todo.pop(0))

    combine_some(5)

    def left(parts):
        coords = []
        for dp, g in parts:
            at = wrapped(ip, dp, n_rp) * n_pb + starts[g]
            c = jnp.broadcast_to(q_all[pl.ds(at, nh)], (nh, RB, LANES))
            coords.append(jnp.where(takes, c, const).reshape(rows, LANES))
        coords = coords[0] if len(coords) == 1 else jnp.concatenate(coords, axis=0)
        return wave(dot(coords[:, :KL].astype(BF16), rmat[...])).astype(BF16)

    sizes = cuts(tiles)
    count = len(sizes)
    firsts = [sum(sizes[:c]) for c in range(count)]
    lanes = [slice(LANES * a, LANES * (a + b)) for a, b in zip(firsts, sizes)]

    def right(c):
        parts = [g_buf[u] for u in range(firsts[c], firsts[c] + sizes[c])]
        return parts[0] if len(parts) == 1 else jnp.concatenate(parts, axis=1)

    def x_copy(dp, g, c):
        part = (pl.ds(g * nh, nh), slice(None), lanes[c])
        return pltpu.make_async_remote_copy(
            src_ref=xsend.at[(dp - 1, *part)], dst_ref=xrecv.at[(dp - 1, *part)],
            send_sem=xs_sem, recv_sem=xr_sem.at[dp - 1, g, c],
            device_id=(wrapped(ip, dp, n_rp), ib), device_id_type=MESH,
        )

    def send_x(dp, g, c, f):
        xsend[dp - 1, g * nh : (g + 1) * nh, :, lanes[c]] = f.reshape(nh, RB, LANES * sizes[c]).astype(BF16)
        x_copy(dp, g, c).start()

    q_waits((n_rp - 1) * nh, 0).wait_recv()
    away = [(dp, 0) for dp in range(1, n_rp)]
    rest = [(dp, 1) for dp in range(1, n_rp)] + [(0, 0), (0, 1)]
    ahead = left(away) if away else None
    pltpu.make_async_copy(g_buf, g_buf, g_sem).wait()
    for c in range(count):
        if away:
            f = dot(ahead, right(c))
            for k, (dp, g) in enumerate(away):
                send_x(dp, g, c, f[k * rows : (k + 1) * rows])

    q_waits(n - 1 - (n_rp - 1) * nh, 1).wait_recv()
    behind = left(rest)
    for c in range(count):
        f = dot(behind, right(c))
        for k, (dp, g) in enumerate(rest):
            block = f[k * rows : (k + 1) * rows]
            if dp == 0:
                own_f[g * nh : (g + 1) * nh, :, lanes[c]] = block.reshape(nh, RB, LANES * sizes[c])
            else:
                send_x(dp, g, c, block)

    def f_copy(b, src, c):
        return pltpu.make_async_remote_copy(
            src_ref=red.at[src, :, lanes[c]], dst_ref=recv.at[ib, :, lanes[c]],
            send_sem=s_sem, recv_sem=r_sem.at[c],
            device_id=(ip, b), device_id_type=MESH,
        )

    def reduce(g, c):
        part = (slice(g * nh, (g + 1) * nh), slice(None), lanes[c])
        total = own_f[part]
        for dp in range(1, n_rp):
            x_copy(dp, g, c).wait_recv()
            total = total + xrecv[(dp - 1, *part)].astype(F32)
        red[part] = total.astype(BF16)
        group(g, lambda b: f_copy(b, b - starts[g] + g * nh, c).start())
        if g == 1:
            recv[ib, :, lanes[c]] = red[nh + ib - near0, :, lanes[c]]

    combine_some(1)
    for c in range(count):
        reduce(0, c)
    combine_some(1)
    for c in range(count):
        reduce(1, c)
        if c % 2 == 0:
            combine_some(1)
    combine_some(tiles)

    sums = [0.0] * qd
    for c in range(count):
        part = (pl.ds(0, n_pb - 1), slice(None), lanes[c])
        pltpu.make_async_remote_copy(
            src_ref=red.at[part], dst_ref=recv.at[part], send_sem=s_sem, recv_sem=r_sem.at[c],
            device_id=partner, device_id_type=MESH,
        ).wait_recv()
        block = recv[:, :, lanes[c]].reshape(half, LANES * sizes[c])
        y = dot(v_left[...], block).astype(BF16)
        for q in range(qd):
            at = 4 * bands * q
            ya, yb = y[at : at + 2 * bands], y[at + 2 * bands : at + 4 * bands]
            pieces = []
            for t in range(sizes[c]):
                cut = slice(LANES * t, LANES * (t + 1))
                pieces += [ya[:, cut], yb[:, cut]]
            w = w_buf[q, 2 * LANES * firsts[c] : 2 * LANES * (firsts[c] + sizes[c]), :]
            sums[q] = sums[q] + dot(jnp.concatenate(pieces, axis=1), w)
    for q in range(qd):
        o_ref[q, 0] = sums[q][:bands]
        o_ref[q, 1] = sums[q][bands:]
    q_waits(n - 1, 0).wait_send()
    if n_rp > 1:
        pltpu.make_async_remote_copy(
            src_ref=xsend, dst_ref=xrecv, send_sem=xs_sem, recv_sem=xr_sem.at[0, 0, 0],
            device_id=partner, device_id_type=MESH,
        ).wait_send()
    part = pl.ds(0, n_pb - 1)
    pltpu.make_async_remote_copy(
        src_ref=red.at[part], dst_ref=recv.at[part], send_sem=s_sem, recv_sem=r_sem.at[0],
        device_id=partner, device_id_type=MESH,
    ).wait_send()


def body(wannier_g, rp_coords, q_coords, k_index, k_vectors, kq_vectors, modes):
    n_rp, n_pb = lax.axis_size("rp"), lax.axis_size("pb")
    n = n_rp * n_pb
    qd = q_coords.shape[1]
    _, local, M, cols = wannier_g.shape
    bands, nu = kq_vectors.shape[2], modes.shape[2]
    RB = -(-(qd * 2 * M) // 8) * 8
    KL = -(-(3 * qd * M + 2 * M) // 16) * 16
    tiles = cols // LANES
    chunks = len(cuts(tiles))
    paired = M == 2
    right = wannier_g if paired else wannier_g.reshape(2 * local * M, cols)
    cfg = (n_rp, n_pb, qd, local, M, cols, bands, nu, RB, KL, paired)
    hbm = pl.BlockSpec(memory_space=pltpu.HBM)
    modes = modes.transpose(0, 2, 1, 3)
    others = max(n_rp - 1, 1)
    return pl.pallas_call(
        functools.partial(kernel, cfg),
        out_shape=pltpu.VMEM((qd, 2, bands, cols), F32),
        in_specs=[hbm] * 7,
        out_specs=pl.BlockSpec(memory_space=pltpu.VMEM),
        scratch_shapes=[
            pltpu.VMEM((tiles, 2 * local * M, LANES), BF16),
            pltpu.SMEM((qd, 3), jnp.int32),
            pltpu.SMEM((1, 1), jnp.int32),
            pltpu.VMEM(rp_coords.shape, jnp.int32),
            pltpu.VMEM(k_vectors.shape, BF16),
            pltpu.VMEM(kq_vectors.shape, BF16),
            pltpu.VMEM(modes.shape, BF16),
            pltpu.VMEM((1, LANES), F32),
            pltpu.VMEM((n, 1, LANES), F32),
            pltpu.VMEM((others, n_pb, RB, cols), BF16),
            pltpu.VMEM((others, n_pb, RB, cols), BF16),
            pltpu.VMEM((n_pb, RB, cols), F32),
            pltpu.VMEM((n_pb, RB, cols), BF16),
            pltpu.VMEM((n_pb, RB, cols), BF16),
            pltpu.VMEM((qd, 2 * cols, cols), BF16),
            pltpu.VMEM((KL, 2 * local * M), BF16),
            pltpu.VMEM((qd * 4 * bands, n_pb * RB), BF16),
            pltpu.SemaphoreType.DMA,
            pltpu.SemaphoreType.DMA((6,)),
            pltpu.SemaphoreType.DMA,
            pltpu.SemaphoreType.DMA((2,)),
            pltpu.SemaphoreType.DMA,
            pltpu.SemaphoreType.DMA((others, 2, chunks)),
            pltpu.SemaphoreType.DMA,
            pltpu.SemaphoreType.DMA((chunks,)),
        ],
        compiler_params=pltpu.CompilerParams(
            collective_id=0, has_side_effects=True, vmem_limit_bytes=60 * 2**20
        ),
    )(right, rp_coords, q_coords.T, k_index.reshape(1, 1), k_vectors, kq_vectors, modes)


def solution(mesh):
    return jax.shard_map(
        body,
        mesh=mesh,
        in_specs=(
            P(None, "rp", "pb", None),
            P(),
            P(None, ("rp", "pb")),
            P(),
            P(),
            P(("rp", "pb"), None, None, None),
            P(("rp", "pb"), None, None, None),
        ),
        out_specs=P(("rp", "pb"), None, None, None),
        check_vma=False,
    )
```

```python
import functools

import jax
import jax.numpy as jnp
import numpy as np
from jax import lax
from jax.experimental import pallas as pl
from jax.experimental.pallas import tpu as pltpu
from jax.sharding import PartitionSpec as P

NK = 16
LANES = 128
MESH = pl.DeviceIdType.MESH
F32 = jnp.float32
BF16 = jnp.bfloat16
ROUND = 1.5 * 2.0**23 * NK
ODD = np.linalg.solve(
    np.array([[h, h**3, h**5, h**7] for h in (1.0, 2.0, 3.0, 4.0)]),
    np.sin(np.pi * np.arange(1, 5) / 8.0),
)


def dot(a, b, dims=((1,), (0,))):
    return lax.dot_general(a, b, (dims, ((), ())), preferred_element_type=F32)


def iota(shape, axis):
    return lax.broadcasted_iota(jnp.int32, shape, axis)


def picks(rows, cols, hit):
    return jnp.where(hit(iota((rows, cols), 0), iota((rows, cols), 1)), 1.0, 0.0).astype(BF16)


def wave(t):
    h = NK // 4 - jnp.abs(t - ((t + ROUND) - ROUND))
    s = h * h
    return h * (ODD[0] + s * (ODD[1] + s * (ODD[2] + s * ODD[3])))


def wrapped(a, b, size):
    c = a + b
    return jnp.where(c >= size, c - size, c)


def cuts(tiles):
    if tiles < 8:
        return [tiles]
    rest = tiles - 2
    return [1] + [rest // 3 + (k == 1) * (rest % 3) for k in range(3)] + [1]


def kernel(
    cfg, g_hbm, rp_hbm, q_hbm, k_hbm, kv_hbm, v_hbm, e_hbm, o_ref,
    g_buf, q_ref, k_ref, rp_ref, kv_ref, v_ref, e_ref, qrow, q_all, xsend, xrecv, own_f, red, recv,
    e_buf, u_buf, rmat, v_left,
    g_sem, in_sem, qs_sem, qr_sem, xs_sem, xr_sem, s_sem, r_sem,
):
    n_rp, n_pb, qd, local, M, cols, bands, nu, RB, KL, paired = cfg
    n = n_rp * n_pb
    ip, ib = lax.axis_index("rp"), lax.axis_index("pb")
    me = ip * n_pb + ib
    depth = local * M
    tiles = cols // LANES
    nh, nq = n_pb // 2, n_pb // 4
    near0 = (ib // nh) * nh
    quarter = ib // nq
    starts = (((quarter + 2) % 4) * nq, (3 - quarter) * nq, near0)
    sizes_of, offsets = (nq, nq, nh), (0, nq, nh)
    OWN = 2

    def group(g, act):
        size = sizes_of[g]

        def one(k, c):
            act(wrapped(ib % size, k, size) + starts[g])
            return c

        lax.fori_loop(int(g == OWN), size, one, 0)

    def to_kind(g, act):
        for dp in range(1, n_rp):
            p = wrapped(ip, dp, n_rp)
            if g == OWN:
                act(p, ib)
            group(g, lambda b, p=p: act(p, b))
        group(g, lambda b: act(ip, b))

    barrier = pltpu.get_barrier_semaphore()
    for g in range(3):
        to_kind(
            g,
            lambda p, b: pl.semaphore_signal(barrier, inc=1, device_id=(p, b), device_id_type=MESH),
        )

    inputs = [
        pltpu.make_async_copy(a, b, in_sem.at[k])
        for k, (a, b) in enumerate(
            (
                (q_hbm, q_ref), (k_hbm, k_ref), (rp_hbm, rp_ref), (kv_hbm, kv_ref),
                (v_hbm, v_ref), (e_hbm, e_ref),
            )
        )
    ]
    for c in inputs:
        c.start()
    flat = g_hbm.reshape(2 * depth, cols) if paired else g_hbm
    for t in range(tiles):
        src = flat.at[:, pl.ds(LANES * t, LANES)]
        pltpu.make_async_copy(src, g_buf.at[t], g_sem).start()

    inputs[0].wait()
    lane = iota((1, LANES), 1)
    row = jnp.zeros((1, LANES), jnp.int32)
    for d in range(3):
        for j in range(qd):
            row = jnp.where(lane // M == d * qd + j, q_ref[j, d], row)
    qrow[...] = (row & (NK - 1)).astype(F32)
    q_all[me] = qrow[...]

    pl.semaphore_wait(barrier, n - 1)

    def q_copy(p, b, kind):
        return pltpu.make_async_remote_copy(
            src_ref=qrow, dst_ref=q_all.at[me], send_sem=qs_sem,
            recv_sem=qr_sem.at[kind], device_id=(p, b), device_id_type=MESH,
        )

    for g in range(3):
        to_kind(g, lambda p, b, g=g: q_copy(p, b, g).start())
    partner = (wrapped(ip, 1 % n_rp, n_rp), ib)

    def q_waits(count, kind):
        part = q_all.at[pl.ds(0, count)]
        return pltpu.make_async_remote_copy(
            src_ref=part, dst_ref=part, send_sem=qs_sem, recv_sem=qr_sem.at[kind],
            device_id=partner, device_id_type=MESH,
        )

    for c in inputs[1:]:
        c.wait()

    own = rp_ref[:, pl.ds(pl.multiple_of(ip * local, LANES), local)] & (NK - 1)
    spread = picks(local, depth, lambda a, b: a == b // M)
    own = dot(own.astype(F32).astype(BF16), spread)
    at = iota((KL, depth), 0)
    same = at % M == iota((KL, depth), 1) % M
    which = at // (qd * M)
    big = jnp.zeros((KL, depth), F32)
    for d in range(3):
        big = jnp.where(which == d, own[d : d + 1, :], big)
    big = jnp.where(same, big, 0.0)
    first = 3 * qd * M
    part = (at - first) // M
    for c in range(2):
        turn = (0.0, 3.0 * NK / 4) if c == 0 else (NK / 4, 0.0)
        turn = jnp.where(same, jnp.where(part == 0, turn[0], turn[1]), NK / 4)
        turn = jnp.where(at < first + 2 * M, turn, 0.0)
        rmat[:, c * depth : (c + 1) * depth] = jnp.where(at < first, big, turn).astype(BF16)

    slot = iota((RB, LANES), 0)
    at = iota((RB, LANES), 1)
    takes = (at < first) & ((at // M) % qd == slot // (2 * M)) & (at % M == slot % M)
    const = jnp.where((slot < qd * 2 * M) & (at - first == slot % (2 * M)), 1.0, 0.0)

    half = n_pb * RB
    slot = iota((bands, half), 1) % RB
    m_of = (iota((bands, half), 1) // RB) * M + slot % M
    pick_m = jnp.where(iota((bands, half), 0) == m_of, 1.0, 0.0).astype(BF16)
    real_in = (slot // M) % 2 == 0
    for q in range(qd):
        a_r, a_i = [dot(v_ref[q, c], pick_m, ((0,), (0,))) for c in range(2)]
        mine = slot // (2 * M) == q
        top = jnp.where(mine, jnp.where(real_in, a_r, a_i), 0.0)
        low = jnp.where(mine, jnp.where(real_in, -a_i, a_r), 0.0)
        v_left[2 * bands * q : 2 * bands * (q + 1), :] = jnp.concatenate([top, low], 0).astype(BF16)

    def reach(t):
        low, high = (LANES * t) // nu, (LANES * (t + 1) - 1) // nu
        return (low * nu) // LANES, ((high + 1) * nu - 1) // LANES + 1

    of_mode_t = picks(nu, cols, lambda b, a: (a - b + nu * bands) % nu == 0)
    of_band_t = picks(bands, cols, lambda b, a: (a >= nu * b) & (a < nu * b + nu))
    unit = kv_ref[k_ref[0, 0]]
    u_right = [dot(unit[c], of_band_t).astype(BF16) for c in range(2)]
    e_right = [[dot(e_ref[q, :, c, :], of_mode_t).astype(BF16) for c in range(2)] for q in range(qd)]
    col = iota((1, cols), 1)
    col_band, col_mode = col // nu, col % nu

    for t in range(tiles):
        lo, hi = reach(t)
        span = slice(LANES * lo, LANES * hi)
        rows_at = iota((LANES, 1), 0) + LANES * t
        row_band = rows_at // nu
        of_mode = picks(LANES, nu, lambda a, b: (a + LANES * t - b + nu * bands) % nu == 0)
        diagonal = row_band == col_band[:, span]
        for q in range(qd):
            for c in range(2):
                e = jnp.where(diagonal, dot(of_mode, e_right[q][c][:, span]), 0.0)
                e_buf[q, (2 * t + c) * LANES : (2 * t + c + 1) * LANES, : LANES * (hi - lo)] = e.astype(BF16)

    def spread_band(t):
        rows_at = iota((LANES, 1), 0) + LANES * t
        of_band = picks(LANES, bands, lambda a, b: (a + LANES * t >= nu * b) & (a + LANES * t < nu * b + nu))
        diagonal = rows_at % nu == col_mode
        for c in range(2):
            u = jnp.where(diagonal, dot(of_band, u_right[c]), 0.0)
            u_buf[(2 * t + c) * LANES : (2 * t + c + 1) * LANES, :] = u.astype(BF16)

    def left(parts):
        coords = []
        for dp, g in parts:
            at, size = wrapped(ip, dp, n_rp) * n_pb + starts[g], sizes_of[g]
            c = jnp.broadcast_to(q_all[pl.ds(at, size)], (size, RB, LANES))
            coords.append(jnp.where(takes, c, const).reshape(size * RB, LANES))
        coords = coords[0] if len(coords) == 1 else jnp.concatenate(coords, axis=0)
        return wave(dot(coords[:, :KL].astype(BF16), rmat[...])).astype(BF16)

    sizes = cuts(tiles)
    count = len(sizes)
    firsts = [sum(sizes[:c]) for c in range(count)]
    lanes = [slice(LANES * a, LANES * (a + b)) for a, b in zip(firsts, sizes)]

    def right(c):
        parts = [g_buf[u] for u in range(firsts[c], firsts[c] + sizes[c])]
        return parts[0] if len(parts) == 1 else jnp.concatenate(parts, axis=1)

    def x_copy(dp, g, c):
        part = (pl.ds(offsets[g], sizes_of[g]), slice(None), lanes[c])
        return pltpu.make_async_remote_copy(
            src_ref=xsend.at[(dp - 1, *part)], dst_ref=xrecv.at[(dp - 1, *part)],
            send_sem=xs_sem, recv_sem=xr_sem.at[dp - 1, g, c],
            device_id=(wrapped(ip, dp, n_rp), ib), device_id_type=MESH,
        )

    def block_of(g, c):
        return slice(offsets[g], offsets[g] + sizes_of[g]), slice(None), lanes[c]

    def emit(g, c, f):
        f = f.reshape(n_rp, sizes_of[g], RB, LANES * sizes[c])
        for dp in range(1, n_rp):
            xsend[(dp - 1, *block_of(g, c))] = f[dp - 1].astype(BF16)
            x_copy(dp, g, c).start()
        own_f[block_of(g, c)] = f[n_rp - 1]

    def fourier(g, then):
        count_of = n_rp * sizes_of[g] - (g == OWN)
        q_waits(count_of, g).wait_recv()
        phases = left([(dp, g) for dp in range(1, n_rp)] + [(0, g)])
        if g == 0:
            pltpu.make_async_copy(g_buf, g_buf, g_sem).wait()
        held = None
        for c in range(count):
            f = dot(phases, right(c))
            if held is not None:
                emit(g, c - 1, held)
                then(c - 1)
            held = f
        emit(g, count - 1, held)
        then(count - 1)

    def f_copy(b, src, c):
        return pltpu.make_async_remote_copy(
            src_ref=red.at[src, :, lanes[c]], dst_ref=recv.at[ib, :, lanes[c]],
            send_sem=s_sem, recv_sem=r_sem.at[c],
            device_id=(ip, b), device_id_type=MESH,
        )

    def reduce(g, c):
        part = block_of(g, c)
        total = own_f[part]
        for dp in range(1, n_rp):
            x_copy(dp, g, c).wait_recv()
            total = total + xrecv[(dp - 1, *part)].astype(F32)
        red[part] = total.astype(BF16)
        group(g, lambda b: f_copy(b, b - starts[g] + offsets[g], c).start())
        if g == OWN:
            recv[ib, :, lanes[c]] = red[offsets[g] + ib - near0, :, lanes[c]]

    early = min(2, count)
    fourier(0, lambda c: None)
    fourier(1, lambda c: None)
    for c in range(early):
        reduce(0, c)
    fourier(2, lambda c: reduce(0, c) if c >= early else None)
    for c in range(count):
        reduce(1, c)
    todo = list(range(tiles))
    for c in range(count):
        for t in todo[: -(-tiles // count)]:
            spread_band(t)
        todo = todo[-(-tiles // count) :]
        reduce(2, c)

    def turned(z):
        parts = []
        for q in range(qd):
            at = 2 * bands * q
            parts += [-z[at + bands : at + 2 * bands], z[at : at + bands]]
        return jnp.concatenate(parts, axis=0)

    total = 0.0
    carry = {}
    done = 0
    held = None

    def by_band(total, pieces, at):
        return total + dot(jnp.concatenate(pieces, axis=1), u_buf[at, :])

    for c in range(count):
        part = (pl.ds(0, n_pb - 1), slice(None), lanes[c])
        pltpu.make_async_remote_copy(
            src_ref=red.at[part], dst_ref=recv.at[part], send_sem=s_sem, recv_sem=r_sem.at[c],
            device_id=partner, device_id_type=MESH,
        ).wait_recv()
        block = recv[:, :, lanes[c]].reshape(half, LANES * sizes[c])
        y = dot(v_left[...], block)
        ya, yb = y.astype(BF16), turned(y).astype(BF16)
        for t in range(firsts[c], firsts[c] + sizes[c]):
            lo, hi = reach(t)
            cut = slice(LANES * (t - firsts[c]), LANES * (t - firsts[c] + 1))
            z = []
            for q in range(qd):
                at = slice(2 * bands * q, 2 * bands * (q + 1))
                y_t = jnp.concatenate([ya[at, cut], yb[at, cut]], axis=1)
                z.append(dot(y_t, e_buf[q, 2 * LANES * t : 2 * LANES * (t + 1), : LANES * (hi - lo)]))
            z = jnp.concatenate(z, axis=0)
            for u in range(lo, hi):
                piece = z[:, LANES * (u - lo) : LANES * (u - lo + 1)]
                carry[u] = carry[u] + piece if u in carry else piece
        whole = LANES * (firsts[c] + sizes[c]) // nu * nu // LANES
        ready = range(done, tiles if c == count - 1 else whole)
        done = max(done, ready.stop)
        if held is not None:
            total = by_band(total, *held)
            held = None
        if len(ready):
            pieces = []
            for u in ready:
                z = carry.pop(u)
                pieces += [z.astype(BF16), turned(z).astype(BF16)]
            at = slice(2 * LANES * ready.start, 2 * LANES * ready.stop)
            held = pieces, at
    total = by_band(total, *held)
    for q in range(qd):
        for c in range(2):
            at = bands * (2 * q + c)
            o_ref[q, c] = total[at : at + bands]
    q_waits(n - 1, 0).wait_send()
    if n_rp > 1:
        pltpu.make_async_remote_copy(
            src_ref=xsend, dst_ref=xrecv, send_sem=xs_sem, recv_sem=xr_sem.at[0, 0, 0],
            device_id=partner, device_id_type=MESH,
        ).wait_send()
    part = pl.ds(0, n_pb - 1)
    pltpu.make_async_remote_copy(
        src_ref=red.at[part], dst_ref=recv.at[part], send_sem=s_sem, recv_sem=r_sem.at[0],
        device_id=partner, device_id_type=MESH,
    ).wait_send()


def body(wannier_g, rp_coords, q_coords, k_index, k_vectors, kq_vectors, modes):
    n_rp, n_pb = lax.axis_size("rp"), lax.axis_size("pb")
    n = n_rp * n_pb
    qd = q_coords.shape[1]
    _, local, M, cols = wannier_g.shape
    bands, nu = kq_vectors.shape[2], modes.shape[2]
    RB = -(-(qd * 2 * M) // 8) * 8
    KL = -(-(3 * qd * M + 2 * M) // 16) * 16
    tiles = cols // LANES
    chunks = len(cuts(tiles))
    paired = M == 2
    right = wannier_g if paired else wannier_g.reshape(2 * local * M, cols)
    cfg = (n_rp, n_pb, qd, local, M, cols, bands, nu, RB, KL, paired)
    hbm = pl.BlockSpec(memory_space=pltpu.HBM)
    modes = modes.transpose(0, 2, 1, 3)
    others = max(n_rp - 1, 1)
    return pl.pallas_call(
        functools.partial(kernel, cfg),
        out_shape=pltpu.VMEM((qd, 2, bands, cols), F32),
        in_specs=[hbm] * 7,
        out_specs=pl.BlockSpec(memory_space=pltpu.VMEM),
        scratch_shapes=[
            pltpu.VMEM((tiles, 2 * local * M, LANES), BF16),
            pltpu.SMEM((qd, 3), jnp.int32),
            pltpu.SMEM((1, 1), jnp.int32),
            pltpu.VMEM(rp_coords.shape, jnp.int32),
            pltpu.VMEM(k_vectors.shape, BF16),
            pltpu.VMEM(kq_vectors.shape, BF16),
            pltpu.VMEM(modes.shape, BF16),
            pltpu.VMEM((1, LANES), F32),
            pltpu.VMEM((n, 1, LANES), F32),
            pltpu.VMEM((others, n_pb, RB, cols), BF16),
            pltpu.VMEM((others, n_pb, RB, cols), BF16),
            pltpu.VMEM((n_pb, RB, cols), F32),
            pltpu.VMEM((n_pb, RB, cols), BF16),
            pltpu.VMEM((n_pb, RB, cols), BF16),
            pltpu.VMEM((qd, 2 * cols, LANES * (-(-LANES // nu) * nu // LANES + 2)), BF16),
            pltpu.VMEM((2 * cols, cols), BF16),
            pltpu.VMEM((KL, 2 * local * M), BF16),
            pltpu.VMEM((qd * 2 * bands, n_pb * RB), BF16),
            pltpu.SemaphoreType.DMA,
            pltpu.SemaphoreType.DMA((6,)),
            pltpu.SemaphoreType.DMA,
            pltpu.SemaphoreType.DMA((3,)),
            pltpu.SemaphoreType.DMA,
            pltpu.SemaphoreType.DMA((others, 3, chunks)),
            pltpu.SemaphoreType.DMA,
            pltpu.SemaphoreType.DMA((chunks,)),
        ],
        compiler_params=pltpu.CompilerParams(
            collective_id=0, has_side_effects=True, vmem_limit_bytes=60 * 2**20
        ),
    )(right, rp_coords, q_coords.T, k_index.reshape(1, 1), k_vectors, kq_vectors, modes)


def solution(mesh):
    return jax.shard_map(
        body,
        mesh=mesh,
        in_specs=(
            P(None, "rp", "pb", None),
            P(),
            P(None, ("rp", "pb")),
            P(),
            P(),
            P(("rp", "pb"), None, None, None),
            P(("rp", "pb"), None, None, None),
        ),
        out_specs=P(("rp", "pb"), None, None, None),
        check_vma=False,
    )
```

```python
import functools

import jax
import jax.numpy as jnp
import numpy as np
from jax import lax
from jax.experimental import pallas as pl
from jax.experimental.pallas import tpu as pltpu
from jax.sharding import PartitionSpec as P

NK = 16
LANES = 128
MESH = pl.DeviceIdType.MESH
F32 = jnp.float32
BF16 = jnp.bfloat16
ROUND = 1.5 * 2.0**23 * NK
ODD = np.linalg.solve(
    np.array([[h, h**3, h**5, h**7] for h in (1.0, 2.0, 3.0, 4.0)]),
    np.sin(np.pi * np.arange(1, 5) / 8.0),
)


def dot(a, b, dims=((1,), (0,))):
    return lax.dot_general(a, b, (dims, ((), ())), preferred_element_type=F32)


def iota(shape, axis):
    return lax.broadcasted_iota(jnp.int32, shape, axis)


def picks(rows, cols, hit):
    return jnp.where(hit(iota((rows, cols), 0), iota((rows, cols), 1)), 1.0, 0.0).astype(BF16)


def wave(t):
    h = NK // 4 - jnp.abs(t - ((t + ROUND) - ROUND))
    s = h * h
    return h * (ODD[0] + s * (ODD[1] + s * (ODD[2] + s * ODD[3])))


def wrapped(a, b, size):
    c = a + b
    return jnp.where(c >= size, c - size, c)


def cuts(tiles):
    if tiles < 8:
        return [tiles]
    return [2] * (tiles // 2) + [1] * (tiles % 2)


def kernel(
    cfg, g_hbm, rp_hbm, q_hbm, k_hbm, kv_hbm, v_hbm, e_hbm, o_ref,
    g_buf, q_ref, k_ref, rp_ref, kv_ref, v_ref, e_ref, qrow, q_all, xsend, xrecv, own_f, red, recv,
    e_buf, u_buf, rmat, v_left,
    g_sem, in_sem, qs_sem, qr_sem, xs_sem, xr_sem, s_sem, r_sem,
):
    n_rp, n_pb, qd, local, M, cols, bands, nu, RB, KL, paired = cfg
    n = n_rp * n_pb
    ip, ib = lax.axis_index("rp"), lax.axis_index("pb")
    me = ip * n_pb + ib
    depth = local * M
    tiles = cols // LANES
    nq = n_pb // 4
    quarter = ib // nq
    near = quarter + 1 - 2 * (quarter % 2)
    starts = [q * nq for q in (quarter, (quarter + 2) % 4, near, 3 - quarter)]
    blocks_of = ((0,), (1,), (2, 3))
    KINDS = 3
    OWN = 0

    def to_block(j, act):
        def one(k, c):
            act(wrapped(ib % nq, k, nq) + starts[j])
            return c

        lax.fori_loop(int(j == OWN), nq, one, 0)

    def to_blocks(blocks, act):
        for j in blocks:
            for dp in range(1, n_rp):
                p = wrapped(ip, dp, n_rp)
                if j == OWN:
                    act(p, ib)
                to_block(j, lambda b, p=p: act(p, b))
            to_block(j, lambda b: act(ip, b))

    barrier = pltpu.get_barrier_semaphore()
    for j in (3, 1, 2, 0):
        to_blocks(
            (j,),
            lambda p, b: pl.semaphore_signal(barrier, inc=1, device_id=(p, b), device_id_type=MESH),
        )

    inputs = [
        pltpu.make_async_copy(a, b, in_sem.at[k])
        for k, (a, b) in enumerate(
            (
                (q_hbm, q_ref), (k_hbm, k_ref), (rp_hbm, rp_ref), (kv_hbm, kv_ref),
                (v_hbm, v_ref), (e_hbm, e_ref),
            )
        )
    ]
    for c in inputs:
        c.start()
    flat = g_hbm.reshape(2 * depth, cols) if paired else g_hbm
    for t in range(tiles):
        src = flat.at[:, pl.ds(LANES * t, LANES)]
        pltpu.make_async_copy(src, g_buf.at[t], g_sem).start()

    inputs[0].wait()
    lane = iota((1, LANES), 1)
    row = jnp.zeros((1, LANES), jnp.int32)
    for d in range(3):
        for j in range(qd):
            row = jnp.where(lane // M == d * qd + j, q_ref[j, d], row)
    qrow[...] = (row & (NK - 1)).astype(F32)
    q_all[me] = qrow[...]

    pl.semaphore_wait(barrier, n - 1)

    def q_copy(p, b, kind):
        return pltpu.make_async_remote_copy(
            src_ref=qrow, dst_ref=q_all.at[me], send_sem=qs_sem,
            recv_sem=qr_sem.at[kind], device_id=(p, b), device_id_type=MESH,
        )

    for g in range(KINDS):
        to_blocks(blocks_of[g], lambda p, b, g=g: q_copy(p, b, g).start())
    partner = (wrapped(ip, 1 % n_rp, n_rp), ib)

    def q_waits(count, kind):
        part = q_all.at[pl.ds(0, count)]
        return pltpu.make_async_remote_copy(
            src_ref=part, dst_ref=part, send_sem=qs_sem, recv_sem=qr_sem.at[kind],
            device_id=partner, device_id_type=MESH,
        )

    for c in inputs[1:]:
        c.wait()

    own = rp_ref[:, pl.ds(pl.multiple_of(ip * local, LANES), local)] & (NK - 1)
    spread = picks(local, depth, lambda a, b: a == b // M)
    own = dot(own.astype(F32).astype(BF16), spread)
    at = iota((KL, depth), 0)
    same = at % M == iota((KL, depth), 1) % M
    which = at // (qd * M)
    big = jnp.zeros((KL, depth), F32)
    for d in range(3):
        big = jnp.where(which == d, own[d : d + 1, :], big)
    big = jnp.where(same, big, 0.0)
    first = 3 * qd * M
    part = (at - first) // M
    for c in range(2):
        turn = (0.0, 3.0 * NK / 4) if c == 0 else (NK / 4, 0.0)
        turn = jnp.where(same, jnp.where(part == 0, turn[0], turn[1]), NK / 4)
        turn = jnp.where(at < first + 2 * M, turn, 0.0)
        rmat[:, c * depth : (c + 1) * depth] = jnp.where(at < first, big, turn).astype(BF16)

    slot = iota((RB, LANES), 0)
    at = iota((RB, LANES), 1)
    takes = (at < first) & ((at // M) % qd == slot // (2 * M)) & (at % M == slot % M)
    const = jnp.where((slot < qd * 2 * M) & (at - first == slot % (2 * M)), 1.0, 0.0)

    half = n_pb * RB
    slot = iota((bands, half), 1) % RB
    m_of = (iota((bands, half), 1) // RB) * M + slot % M
    pick_m = jnp.where(iota((bands, half), 0) == m_of, 1.0, 0.0).astype(BF16)
    real_in = (slot // M) % 2 == 0
    for q in range(qd):
        a_r, a_i = [dot(v_ref[q, c], pick_m, ((0,), (0,))) for c in range(2)]
        mine = slot // (2 * M) == q
        top = jnp.where(mine, jnp.where(real_in, a_r, a_i), 0.0)
        low = jnp.where(mine, jnp.where(real_in, -a_i, a_r), 0.0)
        v_left[2 * bands * q : 2 * bands * (q + 1), :] = jnp.concatenate([top, low], 0).astype(BF16)

    def reach(t):
        low, high = (LANES * t) // nu, (LANES * (t + 1) - 1) // nu
        return (low * nu) // LANES, ((high + 1) * nu - 1) // LANES + 1

    of_mode_t = picks(nu, cols, lambda b, a: (a - b + nu * bands) % nu == 0)
    of_band_t = picks(bands, cols, lambda b, a: (a >= nu * b) & (a < nu * b + nu))
    unit = kv_ref[k_ref[0, 0]]
    u_right = [dot(unit[c], of_band_t).astype(BF16) for c in range(2)]
    e_right = [[dot(e_ref[q, :, c, :], of_mode_t).astype(BF16) for c in range(2)] for q in range(qd)]
    col = iota((1, cols), 1)
    col_band, col_mode = col // nu, col % nu

    for t in range(tiles):
        lo, hi = reach(t)
        span = slice(LANES * lo, LANES * hi)
        rows_at = iota((LANES, 1), 0) + LANES * t
        row_band = rows_at // nu
        of_mode = picks(LANES, nu, lambda a, b: (a + LANES * t - b + nu * bands) % nu == 0)
        diagonal = row_band == col_band[:, span]
        for q in range(qd):
            for c in range(2):
                e = jnp.where(diagonal, dot(of_mode, e_right[q][c][:, span]), 0.0)
                e_buf[q, (2 * t + c) * LANES : (2 * t + c + 1) * LANES, : LANES * (hi - lo)] = e.astype(BF16)

    def spread_band(t):
        rows_at = iota((LANES, 1), 0) + LANES * t
        of_band = picks(LANES, bands, lambda a, b: (a + LANES * t >= nu * b) & (a + LANES * t < nu * b + nu))
        diagonal = rows_at % nu == col_mode
        for c in range(2):
            u = jnp.where(diagonal, dot(of_band, u_right[c]), 0.0)
            u_buf[(2 * t + c) * LANES : (2 * t + c + 1) * LANES, :] = u.astype(BF16)

    def left(parts):
        coords = []
        for dp, j in parts:
            at = wrapped(ip, dp, n_rp) * n_pb + starts[j]
            c = jnp.broadcast_to(q_all[pl.ds(at, nq)], (nq, RB, LANES))
            coords.append(jnp.where(takes, c, const).reshape(nq * RB, LANES))
        coords = coords[0] if len(coords) == 1 else jnp.concatenate(coords, axis=0)
        return wave(dot(coords[:, :KL].astype(BF16), rmat[...])).astype(BF16)

    sizes = cuts(tiles)
    count = len(sizes)
    firsts = [sum(sizes[:c]) for c in range(count)]
    lanes = [slice(LANES * a, LANES * (a + b)) for a, b in zip(firsts, sizes)]

    def right(c):
        parts = [g_buf[u] for u in range(firsts[c], firsts[c] + sizes[c])]
        return parts[0] if len(parts) == 1 else jnp.concatenate(parts, axis=1)

    def x_copy(dp, g, c):
        part = (pl.ds(nq * blocks_of[g][0], nq * len(blocks_of[g])), slice(None), lanes[c])
        return pltpu.make_async_remote_copy(
            src_ref=xsend.at[(dp - 1, *part)], dst_ref=xrecv.at[(dp - 1, *part)],
            send_sem=xs_sem, recv_sem=xr_sem.at[dp - 1, g, c],
            device_id=(wrapped(ip, dp, n_rp), ib), device_id_type=MESH,
        )

    def block_of(g, c):
        return slice(nq * blocks_of[g][0], nq * (blocks_of[g][-1] + 1)), slice(None), lanes[c]

    def emit(g, c, f):
        f = f.reshape(n_rp, nq * len(blocks_of[g]), RB, LANES * sizes[c])
        for dp in range(1, n_rp):
            xsend[(dp - 1, *block_of(g, c))] = f[dp - 1].astype(BF16)
            x_copy(dp, g, c).start()
        own_f[block_of(g, c)] = f[n_rp - 1]

    phases = {}

    def phase(g):
        count_of = n_rp * nq * len(blocks_of[g]) - (OWN in blocks_of[g])
        q_waits(count_of, g).wait_recv()
        phases[g] = left([(dp, j) for dp in [*range(1, n_rp), 0] for j in blocks_of[g]])

    def fourier(g, chunks, then=lambda c: None):
        held = None
        for c in chunks:
            f = dot(phases[g], right(c))
            if held is not None:
                emit(g, *held)
                then(held[0])
            held = c, f
        if held is not None:
            emit(g, *held)
            then(held[0])

    def f_copy(b, src, c):
        return pltpu.make_async_remote_copy(
            src_ref=red.at[src, :, lanes[c]], dst_ref=recv.at[ib, :, lanes[c]],
            send_sem=s_sem, recv_sem=r_sem.at[c],
            device_id=(ip, b), device_id_type=MESH,
        )

    def reduce(g, c):
        part = block_of(g, c)
        total = own_f[part]
        for dp in range(1, n_rp):
            x_copy(dp, g, c).wait_recv()
            total = total + xrecv[(dp - 1, *part)].astype(F32)
        red[part] = total.astype(BF16)
        for j in blocks_of[g]:
            to_block(j, lambda b, j=j: f_copy(b, b - starts[j] + nq * j, c).start())
            if j == OWN:
                recv[ib, :, lanes[c]] = red[nq * j + ib % nq, :, lanes[c]]

    ahead = count - 2 if count > 2 else count
    phase(0)
    pltpu.make_async_copy(g_buf, g_buf, g_sem).wait()
    fourier(0, range(ahead))
    phase(1)
    fourier(1, range(count))
    fourier(0, range(ahead, count))
    phase(2)
    todo = [functools.partial(reduce, g, c) for g in (1, 0) for c in range(count)]
    fourier(2, range(count), lambda c: todo.pop(0)() if c >= 2 else None)
    for act in todo:
        act()
    bands_left = list(range(tiles))

    def spread_some(most):
        for _ in range(min(most, len(bands_left))):
            spread_band(bands_left.pop(0))

    for c in range(count):
        spread_some(4 if c == 0 else 1)
        reduce(2, c)
    spread_some(tiles)

    def turned(z):
        parts = []
        for q in range(qd):
            at = 2 * bands * q
            parts += [-z[at + bands : at + 2 * bands], z[at : at + bands]]
        return jnp.concatenate(parts, axis=0)

    total = 0.0
    carry = {}
    done = 0
    held = None

    def by_band(total, pieces, at):
        return total + dot(jnp.concatenate(pieces, axis=1), u_buf[at, :])

    for c in range(count):
        part = (pl.ds(0, n_pb - 1), slice(None), lanes[c])
        pltpu.make_async_remote_copy(
            src_ref=red.at[part], dst_ref=recv.at[part], send_sem=s_sem, recv_sem=r_sem.at[c],
            device_id=partner, device_id_type=MESH,
        ).wait_recv()
        block = recv[:, :, lanes[c]].reshape(half, LANES * sizes[c])
        y = dot(v_left[...], block)
        ya, yb = y.astype(BF16), turned(y).astype(BF16)
        for t in range(firsts[c], firsts[c] + sizes[c]):
            lo, hi = reach(t)
            cut = slice(LANES * (t - firsts[c]), LANES * (t - firsts[c] + 1))
            z = []
            for q in range(qd):
                at = slice(2 * bands * q, 2 * bands * (q + 1))
                y_t = jnp.concatenate([ya[at, cut], yb[at, cut]], axis=1)
                z.append(dot(y_t, e_buf[q, 2 * LANES * t : 2 * LANES * (t + 1), : LANES * (hi - lo)]))
            z = jnp.concatenate(z, axis=0)
            for u in range(lo, hi):
                piece = z[:, LANES * (u - lo) : LANES * (u - lo + 1)]
                carry[u] = carry[u] + piece if u in carry else piece
        whole = LANES * (firsts[c] + sizes[c]) // nu * nu // LANES
        ready = range(done, tiles if c == count - 1 else whole)
        done = max(done, ready.stop)
        if held is not None:
            total = by_band(total, *held)
            held = None
        if len(ready):
            pieces = []
            for u in ready:
                z = carry.pop(u)
                pieces += [z.astype(BF16), turned(z).astype(BF16)]
            at = slice(2 * LANES * ready.start, 2 * LANES * ready.stop)
            held = pieces, at
    total = by_band(total, *held)
    for q in range(qd):
        for c in range(2):
            at = bands * (2 * q + c)
            o_ref[q, c] = total[at : at + bands]
    q_waits(n - 1, 0).wait_send()
    if n_rp > 1:
        pltpu.make_async_remote_copy(
            src_ref=xsend, dst_ref=xrecv, send_sem=xs_sem, recv_sem=xr_sem.at[0, 0, 0],
            device_id=partner, device_id_type=MESH,
        ).wait_send()
    part = pl.ds(0, n_pb - 1)
    pltpu.make_async_remote_copy(
        src_ref=red.at[part], dst_ref=recv.at[part], send_sem=s_sem, recv_sem=r_sem.at[0],
        device_id=partner, device_id_type=MESH,
    ).wait_send()


def body(wannier_g, rp_coords, q_coords, k_index, k_vectors, kq_vectors, modes):
    n_rp, n_pb = lax.axis_size("rp"), lax.axis_size("pb")
    n = n_rp * n_pb
    qd = q_coords.shape[1]
    _, local, M, cols = wannier_g.shape
    bands, nu = kq_vectors.shape[2], modes.shape[2]
    RB = -(-(qd * 2 * M) // 8) * 8
    KL = -(-(3 * qd * M + 2 * M) // 16) * 16
    tiles = cols // LANES
    chunks = len(cuts(tiles))
    paired = M == 2
    right = wannier_g if paired else wannier_g.reshape(2 * local * M, cols)
    cfg = (n_rp, n_pb, qd, local, M, cols, bands, nu, RB, KL, paired)
    hbm = pl.BlockSpec(memory_space=pltpu.HBM)
    modes = modes.transpose(0, 2, 1, 3)
    others = max(n_rp - 1, 1)
    return pl.pallas_call(
        functools.partial(kernel, cfg),
        out_shape=pltpu.VMEM((qd, 2, bands, cols), F32),
        in_specs=[hbm] * 7,
        out_specs=pl.BlockSpec(memory_space=pltpu.VMEM),
        scratch_shapes=[
            pltpu.VMEM((tiles, 2 * local * M, LANES), BF16),
            pltpu.SMEM((qd, 3), jnp.int32),
            pltpu.SMEM((1, 1), jnp.int32),
            pltpu.VMEM(rp_coords.shape, jnp.int32),
            pltpu.VMEM(k_vectors.shape, BF16),
            pltpu.VMEM(kq_vectors.shape, BF16),
            pltpu.VMEM(modes.shape, BF16),
            pltpu.VMEM((1, LANES), F32),
            pltpu.VMEM((n, 1, LANES), F32),
            pltpu.VMEM((others, n_pb, RB, cols), BF16),
            pltpu.VMEM((others, n_pb, RB, cols), BF16),
            pltpu.VMEM((n_pb, RB, cols), F32),
            pltpu.VMEM((n_pb, RB, cols), BF16),
            pltpu.VMEM((n_pb, RB, cols), BF16),
            pltpu.VMEM((qd, 2 * cols, LANES * (-(-LANES // nu) * nu // LANES + 2)), BF16),
            pltpu.VMEM((2 * cols, cols), BF16),
            pltpu.VMEM((KL, 2 * local * M), BF16),
            pltpu.VMEM((qd * 2 * bands, n_pb * RB), BF16),
            pltpu.SemaphoreType.DMA,
            pltpu.SemaphoreType.DMA((6,)),
            pltpu.SemaphoreType.DMA,
            pltpu.SemaphoreType.DMA((3,)),
            pltpu.SemaphoreType.DMA,
            pltpu.SemaphoreType.DMA((others, 3, chunks)),
            pltpu.SemaphoreType.DMA,
            pltpu.SemaphoreType.DMA((chunks,)),
        ],
        compiler_params=pltpu.CompilerParams(
            collective_id=0, has_side_effects=True, vmem_limit_bytes=60 * 2**20
        ),
    )(right, rp_coords, q_coords.T, k_index.reshape(1, 1), k_vectors, kq_vectors, modes)


def solution(mesh):
    return jax.shard_map(
        body,
        mesh=mesh,
        in_specs=(
            P(None, "rp", "pb", None),
            P(),
            P(None, ("rp", "pb")),
            P(),
            P(),
            P(("rp", "pb"), None, None, None),
            P(("rp", "pb"), None, None, None),
        ),
        out_specs=P(("rp", "pb"), None, None, None),
        check_vma=False,
    )
```

```python
import functools

import jax
import jax.numpy as jnp
import numpy as np
from jax import lax
from jax.experimental import pallas as pl
from jax.experimental.pallas import tpu as pltpu
from jax.sharding import PartitionSpec as P

NK = 16
LANES = 128
MESH = pl.DeviceIdType.MESH
F32 = jnp.float32
BF16 = jnp.bfloat16
ROUND = 1.5 * 2.0**23 * NK
ODD = np.linalg.solve(
    np.array([[h, h**3, h**5, h**7] for h in (1.0, 2.0, 3.0, 4.0)]),
    np.sin(np.pi * np.arange(1, 5) / 8.0),
)


def dot(a, b, dims=((1,), (0,))):
    return lax.dot_general(a, b, (dims, ((), ())), preferred_element_type=F32)


def iota(shape, axis):
    return lax.broadcasted_iota(jnp.int32, shape, axis)


def picks(rows, cols, hit):
    return jnp.where(hit(iota((rows, cols), 0), iota((rows, cols), 1)), 1.0, 0.0).astype(BF16)


def wave(t):
    h = NK // 4 - jnp.abs(t - ((t + ROUND) - ROUND))
    s = h * h
    return h * (ODD[0] + s * (ODD[1] + s * (ODD[2] + s * ODD[3])))


def wrapped(a, b, size):
    c = a + b
    return jnp.where(c >= size, c - size, c)


def cuts(tiles):
    if tiles < 8:
        return [tiles]
    return [2] * (tiles // 2) + [1] * (tiles % 2)


def kernel(
    cfg, g_hbm, rp_hbm, q_hbm, k_hbm, kv_hbm, v_hbm, e_hbm, o_ref,
    g_buf, q_ref, k_ref, rp_ref, kv_ref, v_ref, e_ref, qrow, q_all, xsend, xrecv, own_f, red, recv,
    e_buf, u_buf, rmat, v_left,
    g_sem, in_sem, qs_sem, qr_sem, xs_sem, xr_sem, s_sem, r_sem,
):
    n_rp, n_pb, qd, local, M, cols, bands, nu, RB, KL, paired = cfg
    n = n_rp * n_pb
    ip, ib = lax.axis_index("rp"), lax.axis_index("pb")
    me = ip * n_pb + ib
    depth = local * M
    tiles = cols // LANES
    nq = n_pb // 4
    quarter = ib // nq
    near = quarter + 1 - 2 * (quarter % 2)
    starts = [q * nq for q in (quarter, (quarter + 2) % 4, near, 3 - quarter)]
    blocks_of = ((0,), (1,), (2, 3))
    KINDS = 3
    OWN = 0

    def to_block(j, act):
        def one(k, c):
            act(wrapped(ib % nq, k, nq) + starts[j])
            return c

        lax.fori_loop(int(j == OWN), nq, one, 0)

    def to_blocks(blocks, act):
        for j in blocks:
            for dp in range(1, n_rp):
                p = wrapped(ip, dp, n_rp)
                if j == OWN:
                    act(p, ib)
                to_block(j, lambda b, p=p: act(p, b))
            to_block(j, lambda b: act(ip, b))

    barrier = pltpu.get_barrier_semaphore()
    for j in (3, 1, 2, 0):
        to_blocks(
            (j,),
            lambda p, b: pl.semaphore_signal(barrier, inc=1, device_id=(p, b), device_id_type=MESH),
        )

    inputs = [
        pltpu.make_async_copy(a, b, in_sem.at[k])
        for k, (a, b) in enumerate(
            (
                (q_hbm, q_ref), (k_hbm, k_ref), (rp_hbm, rp_ref), (kv_hbm, kv_ref),
                (v_hbm, v_ref), (e_hbm, e_ref),
            )
        )
    ]
    for c in inputs:
        c.start()
    flat = g_hbm.reshape(2 * depth, cols) if paired else g_hbm
    for t in range(tiles):
        src = flat.at[:, pl.ds(LANES * t, LANES)]
        pltpu.make_async_copy(src, g_buf.at[t], g_sem).start()

    inputs[0].wait()
    lane = iota((1, LANES), 1)
    row = jnp.zeros((1, LANES), jnp.int32)
    for d in range(3):
        for j in range(qd):
            row = jnp.where(lane // M == d * qd + j, q_ref[j, d], row)
    qrow[...] = (row & (NK - 1)).astype(F32)
    q_all[me] = qrow[...]

    pl.semaphore_wait(barrier, n - 1)

    def q_copy(p, b, kind):
        return pltpu.make_async_remote_copy(
            src_ref=qrow, dst_ref=q_all.at[me], send_sem=qs_sem,
            recv_sem=qr_sem.at[kind], device_id=(p, b), device_id_type=MESH,
        )

    for g in range(KINDS):
        to_blocks(blocks_of[g], lambda p, b, g=g: q_copy(p, b, g).start())
    partner = (wrapped(ip, 1 % n_rp, n_rp), ib)

    def q_waits(count, kind):
        part = q_all.at[pl.ds(0, count)]
        return pltpu.make_async_remote_copy(
            src_ref=part, dst_ref=part, send_sem=qs_sem, recv_sem=qr_sem.at[kind],
            device_id=partner, device_id_type=MESH,
        )

    for c in inputs[1:]:
        c.wait()

    own = rp_ref[:, pl.ds(pl.multiple_of(ip * local, LANES), local)] & (NK - 1)
    spread = picks(local, depth, lambda a, b: a == b // M)
    own = dot(own.astype(F32).astype(BF16), spread)
    at = iota((KL, depth), 0)
    same = at % M == iota((KL, depth), 1) % M
    which = at // (qd * M)
    big = jnp.zeros((KL, depth), F32)
    for d in range(3):
        big = jnp.where(which == d, own[d : d + 1, :], big)
    big = jnp.where(same, big, 0.0)
    first = 3 * qd * M
    part = (at - first) // M
    for c in range(2):
        turn = (0.0, 3.0 * NK / 4) if c == 0 else (NK / 4, 0.0)
        turn = jnp.where(same, jnp.where(part == 0, turn[0], turn[1]), NK / 4)
        turn = jnp.where(at < first + 2 * M, turn, 0.0)
        rmat[:, c * depth : (c + 1) * depth] = jnp.where(at < first, big, turn).astype(BF16)

    slot = iota((RB, LANES), 0)
    at = iota((RB, LANES), 1)
    takes = (at < first) & ((at // M) % qd == slot // (2 * M)) & (at % M == slot % M)
    const = jnp.where((slot < qd * 2 * M) & (at - first == slot % (2 * M)), 1.0, 0.0)

    half = n_pb * RB
    slot = iota((bands, half), 1) % RB
    m_of = (iota((bands, half), 1) // RB) * M + slot % M
    pick_m = jnp.where(iota((bands, half), 0) == m_of, 1.0, 0.0).astype(BF16)
    real_in = (slot // M) % 2 == 0
    for q in range(qd):
        a_r, a_i = [dot(v_ref[q, c], pick_m, ((0,), (0,))) for c in range(2)]
        mine = slot // (2 * M) == q
        top = jnp.where(mine, jnp.where(real_in, a_r, a_i), 0.0)
        low = jnp.where(mine, jnp.where(real_in, -a_i, a_r), 0.0)
        v_left[2 * bands * q : 2 * bands * (q + 1), :] = jnp.concatenate([top, low], 0).astype(BF16)

    def reach(t):
        low, high = (LANES * t) // nu, (LANES * (t + 1) - 1) // nu
        return (low * nu) // LANES, ((high + 1) * nu - 1) // LANES + 1

    of_mode_t = picks(nu, cols, lambda b, a: (a - b + nu * bands) % nu == 0)
    of_band_t = picks(bands, cols, lambda b, a: (a >= nu * b) & (a < nu * b + nu))
    unit = kv_ref[k_ref[0, 0]]
    u_right = [dot(unit[c], of_band_t).astype(BF16) for c in range(2)]
    e_right = [[dot(e_ref[q, :, c, :], of_mode_t).astype(BF16) for c in range(2)] for q in range(qd)]
    col = iota((1, cols), 1)
    col_band, col_mode = col // nu, col % nu

    for t in range(tiles):
        lo, hi = reach(t)
        span = slice(LANES * lo, LANES * hi)
        rows_at = iota((LANES, 1), 0) + LANES * t
        row_band = rows_at // nu
        of_mode = picks(LANES, nu, lambda a, b: (a + LANES * t - b + nu * bands) % nu == 0)
        diagonal = row_band == col_band[:, span]
        for q in range(qd):
            for c in range(2):
                e = jnp.where(diagonal, dot(of_mode, e_right[q][c][:, span]), 0.0)
                e_buf[q, (2 * t + c) * LANES : (2 * t + c + 1) * LANES, : LANES * (hi - lo)] = e.astype(BF16)

    def spread_band(t):
        rows_at = iota((LANES, 1), 0) + LANES * t
        of_band = picks(LANES, bands, lambda a, b: (a + LANES * t >= nu * b) & (a + LANES * t < nu * b + nu))
        diagonal = rows_at % nu == col_mode
        for c in range(2):
            u = jnp.where(diagonal, dot(of_band, u_right[c]), 0.0)
            u_buf[(2 * t + c) * LANES : (2 * t + c + 1) * LANES, :] = u.astype(BF16)

    def left(parts):
        coords = []
        for dp, j in parts:
            at = wrapped(ip, dp, n_rp) * n_pb + starts[j]
            c = jnp.broadcast_to(q_all[pl.ds(at, nq)], (nq, RB, LANES))
            coords.append(jnp.where(takes, c, const).reshape(nq * RB, LANES))
        coords = coords[0] if len(coords) == 1 else jnp.concatenate(coords, axis=0)
        return wave(dot(coords[:, :KL].astype(BF16), rmat[...])).astype(BF16)

    sizes = cuts(tiles)
    count = len(sizes)
    firsts = [sum(sizes[:c]) for c in range(count)]
    lanes = [slice(LANES * a, LANES * (a + b)) for a, b in zip(firsts, sizes)]

    def right(c):
        parts = [g_buf[u] for u in range(firsts[c], firsts[c] + sizes[c])]
        return parts[0] if len(parts) == 1 else jnp.concatenate(parts, axis=1)

    def x_copy(dp, g, c):
        part = (pl.ds(nq * blocks_of[g][0], nq * len(blocks_of[g])), slice(None), lanes[c])
        return pltpu.make_async_remote_copy(
            src_ref=xsend.at[(dp - 1, *part)], dst_ref=xrecv.at[(dp - 1, *part)],
            send_sem=xs_sem, recv_sem=xr_sem.at[dp - 1, g, c],
            device_id=(wrapped(ip, dp, n_rp), ib), device_id_type=MESH,
        )

    def block_of(g, c):
        return slice(nq * blocks_of[g][0], nq * (blocks_of[g][-1] + 1)), slice(None), lanes[c]

    def emit(g, c, f):
        f = f.reshape(n_rp, nq * len(blocks_of[g]), RB, LANES * sizes[c])
        for dp in range(1, n_rp):
            xsend[(dp - 1, *block_of(g, c))] = f[dp - 1].astype(BF16)
            x_copy(dp, g, c).start()
        own_f[block_of(g, c)] = f[n_rp - 1]

    phases = {}

    def phase(g):
        count_of = n_rp * nq * len(blocks_of[g]) - (OWN in blocks_of[g])
        q_waits(count_of, g).wait_recv()
        phases[g] = left([(dp, j) for dp in [*range(1, n_rp), 0] for j in blocks_of[g]])

    def fourier(g, chunks, then=lambda c: None):
        held = None
        for c in chunks:
            f = dot(phases[g], right(c))
            if held is not None:
                emit(g, *held)
                then(held[0])
            held = c, f
        if held is not None:
            emit(g, *held)
            then(held[0])

    def f_copy(b, src, c):
        return pltpu.make_async_remote_copy(
            src_ref=red.at[src, :, lanes[c]], dst_ref=recv.at[ib, :, lanes[c]],
            send_sem=s_sem, recv_sem=r_sem.at[c],
            device_id=(ip, b), device_id_type=MESH,
        )

    def reduce(g, c):
        part = block_of(g, c)
        total = own_f[part]
        for dp in range(1, n_rp):
            x_copy(dp, g, c).wait_recv()
            total = total + xrecv[(dp - 1, *part)].astype(F32)
        red[part] = total.astype(BF16)
        for j in blocks_of[g]:
            to_block(j, lambda b, j=j: f_copy(b, b - starts[j] + nq * j, c).start())
            if j == OWN:
                recv[ib, :, lanes[c]] = red[nq * j + ib % nq, :, lanes[c]]

    ahead = count - 2 if count > 2 else count
    phase(0)
    pltpu.make_async_copy(g_buf, g_buf, g_sem).wait()
    fourier(0, range(ahead))
    phase(1)
    fourier(1, range(count))
    fourier(0, range(ahead, count))
    phase(2)
    todo = [functools.partial(reduce, g, c) for g in (1, 0) for c in range(count)]
    fourier(2, range(count), lambda c: todo.pop(0)() if c >= 1 else None)
    for act in todo:
        act()
    bands_left = list(range(tiles))

    def spread_some(most):
        for _ in range(min(most, len(bands_left))):
            spread_band(bands_left.pop(0))

    for c in range(count):
        spread_some(4 if c == 0 else 1)
        reduce(2, c)
    spread_some(tiles)

    def turned(z):
        parts = []
        for q in range(qd):
            at = 2 * bands * q
            parts += [-z[at + bands : at + 2 * bands], z[at : at + bands]]
        return jnp.concatenate(parts, axis=0)

    carry = {}

    def by_mode(c):
        block = recv[:, :, lanes[c]].reshape(half, LANES * sizes[c])
        y = dot(v_left[...], block)
        ya, yb = y.astype(BF16), turned(y).astype(BF16)
        for t in range(firsts[c], firsts[c] + sizes[c]):
            lo, hi = reach(t)
            cut = slice(LANES * (t - firsts[c]), LANES * (t - firsts[c] + 1))
            z = []
            for q in range(qd):
                at = slice(2 * bands * q, 2 * bands * (q + 1))
                y_t = jnp.concatenate([ya[at, cut], yb[at, cut]], axis=1)
                z.append(dot(y_t, e_buf[q, 2 * LANES * t : 2 * LANES * (t + 1), : LANES * (hi - lo)]))
            z = jnp.concatenate(z, axis=0)
            for u in range(lo, hi):
                piece = z[:, LANES * (u - lo) : LANES * (u - lo + 1)]
                carry[u] = carry[u] + piece if u in carry else piece

    def by_band(first, last):
        pieces = []
        for u in range(first, last):
            z = carry.pop(u)
            pieces += [z.astype(BF16), turned(z).astype(BF16)]
        return dot(jnp.concatenate(pieces, axis=1), u_buf[2 * LANES * first : 2 * LANES * last, :])

    rounds = [[c] for c in range(count - 2)] + [list(range(max(count - 2, 0), count))]
    total = 0.0
    done = 0
    whole = 0
    for k, chunks in enumerate(rounds):
        for c in chunks:
            part = (pl.ds(0, n_pb - 1), slice(None), lanes[c])
            pltpu.make_async_remote_copy(
                src_ref=red.at[part], dst_ref=recv.at[part], send_sem=s_sem, recv_sem=r_sem.at[c],
                device_id=partner, device_id_type=MESH,
            ).wait_recv()
        for c in chunks:
            by_mode(c)
        final = k == len(rounds) - 1
        if not final:
            whole = LANES * (firsts[chunks[-1]] + sizes[chunks[-1]]) // nu * nu // LANES
        if whole > done and (final or (whole - done > 2 and k < len(rounds) - 2)):
            total = total + by_band(done, whole)
            done = whole
    total = total + by_band(done, tiles)
    for q in range(qd):
        for c in range(2):
            at = bands * (2 * q + c)
            o_ref[q, c] = total[at : at + bands]
    q_waits(n - 1, 0).wait_send()
    if n_rp > 1:
        pltpu.make_async_remote_copy(
            src_ref=xsend, dst_ref=xrecv, send_sem=xs_sem, recv_sem=xr_sem.at[0, 0, 0],
            device_id=partner, device_id_type=MESH,
        ).wait_send()
    part = pl.ds(0, n_pb - 1)
    pltpu.make_async_remote_copy(
        src_ref=red.at[part], dst_ref=recv.at[part], send_sem=s_sem, recv_sem=r_sem.at[0],
        device_id=partner, device_id_type=MESH,
    ).wait_send()


def body(wannier_g, rp_coords, q_coords, k_index, k_vectors, kq_vectors, modes):
    n_rp, n_pb = lax.axis_size("rp"), lax.axis_size("pb")
    n = n_rp * n_pb
    qd = q_coords.shape[1]
    _, local, M, cols = wannier_g.shape
    bands, nu = kq_vectors.shape[2], modes.shape[2]
    RB = -(-(qd * 2 * M) // 8) * 8
    KL = -(-(3 * qd * M + 2 * M) // 16) * 16
    tiles = cols // LANES
    chunks = len(cuts(tiles))
    paired = M == 2
    right = wannier_g if paired else wannier_g.reshape(2 * local * M, cols)
    cfg = (n_rp, n_pb, qd, local, M, cols, bands, nu, RB, KL, paired)
    hbm = pl.BlockSpec(memory_space=pltpu.HBM)
    modes = modes.transpose(0, 2, 1, 3)
    others = max(n_rp - 1, 1)
    return pl.pallas_call(
        functools.partial(kernel, cfg),
        out_shape=pltpu.VMEM((qd, 2, bands, cols), F32),
        in_specs=[hbm] * 7,
        out_specs=pl.BlockSpec(memory_space=pltpu.VMEM),
        scratch_shapes=[
            pltpu.VMEM((tiles, 2 * local * M, LANES), BF16),
            pltpu.SMEM((qd, 3), jnp.int32),
            pltpu.SMEM((1, 1), jnp.int32),
            pltpu.VMEM(rp_coords.shape, jnp.int32),
            pltpu.VMEM(k_vectors.shape, BF16),
            pltpu.VMEM(kq_vectors.shape, BF16),
            pltpu.VMEM(modes.shape, BF16),
            pltpu.VMEM((1, LANES), F32),
            pltpu.VMEM((n, 1, LANES), F32),
            pltpu.VMEM((others, n_pb, RB, cols), BF16),
            pltpu.VMEM((others, n_pb, RB, cols), BF16),
            pltpu.VMEM((n_pb, RB, cols), F32),
            pltpu.VMEM((n_pb, RB, cols), BF16),
            pltpu.VMEM((n_pb, RB, cols), BF16),
            pltpu.VMEM((qd, 2 * cols, LANES * (-(-LANES // nu) * nu // LANES + 2)), BF16),
            pltpu.VMEM((2 * cols, cols), BF16),
            pltpu.VMEM((KL, 2 * local * M), BF16),
            pltpu.VMEM((qd * 2 * bands, n_pb * RB), BF16),
            pltpu.SemaphoreType.DMA,
            pltpu.SemaphoreType.DMA((6,)),
            pltpu.SemaphoreType.DMA,
            pltpu.SemaphoreType.DMA((3,)),
            pltpu.SemaphoreType.DMA,
            pltpu.SemaphoreType.DMA((others, 3, chunks)),
            pltpu.SemaphoreType.DMA,
            pltpu.SemaphoreType.DMA((chunks,)),
        ],
        compiler_params=pltpu.CompilerParams(
            collective_id=0, has_side_effects=True, vmem_limit_bytes=60 * 2**20
        ),
    )(right, rp_coords, q_coords.T, k_index.reshape(1, 1), k_vectors, kq_vectors, modes)


def solution(mesh):
    return jax.shard_map(
        body,
        mesh=mesh,
        in_specs=(
            P(None, "rp", "pb", None),
            P(),
            P(None, ("rp", "pb")),
            P(),
            P(),
            P(("rp", "pb"), None, None, None),
            P(("rp", "pb"), None, None, None),
        ),
        out_specs=P(("rp", "pb"), None, None, None),
        check_vma=False,
    )
```
